128 devices in a mesh: row: 8 (over y, z_hi), col: 16 (over z_lo, x, core).
Axes of the slice: x: 4, y: 4, z: 4 (z_hi: 2, z_lo: 2; z = z_hi * 2 + z_lo), core: 2. Of those that a mesh axis runs over, the one named last changes fastest.
Arguments:
- inverse: float32 [24576, 24576], P('row', 'col'), may hold values from -0.0546875 to 0.0546875
- parent_panel: float32 [24576, 256], P(('row', 'col')), may hold values from -1.8 to 1.8
- child_panel: float32 [24576, 256], P(('row', 'col')), may hold values from -1.8 to 1.8
- child_top: float32 [256, 256], replicated, may hold values from -0.375 to 0.375
- diag_parent: float32 [256, 256], replicated, may hold values from -12 to 12
- diag_child: float32 [256, 256], replicated, may hold values from -12 to 12
- parent_blocks: int32 [192], replicated, may hold values from 0 to 1
- child_blocks: int32 [192], replicated, may hold values from 0 to 1, as said below
Outputs:
- parent_column: float32 [24576, 256], P(('row', 'col'))
- parent_diagonal: float32 [256, 256], replicated
- child_column: float32 [24576, 256], P(('row', 'col'))
- child_upper: float32 [256, 256], replicated
- child_diagonal: float32 [256, 256], replicated
The draws below stay inside these ranges and needn't reach their ends.
Inputs may be any that keep to these rules, and one draw needn't show every extreme that they name: `child_blocks`: each entry is 0 or 1, and is 1 only where parent_blocks is 1.
All inputs are finite; a program needn't handle non-finite values.
Results may differ from the reference program's by a relative error of at most 0.000086.
Values sent between devices are 32-bit elements; how exact they have to be, the bound alone decides.
No kernel may reach another device: no remote copies, remote signals or barrier semaphores. Data moves between devices by JAX's collectives and lax.ppermute only.
A program may use at most 128 MiB of HBM per device.

```python
import jax
import jax.numpy as jnp
from jax import lax

M = 24576
W = 256
BLK = 128
NBLK = 192


def structure_flags(key):
    base_key = jax.random.fold_in(key, 11)
    first_key, second_key = jax.random.split(base_key)
    parent_flags = jnp.where(jax.random.randint(first_key, (NBLK,), 0, 3) > 0, 1, 0).astype(jnp.int32)
    keep_flags = jax.random.randint(second_key, (NBLK,), 0, 2).astype(jnp.int32)
    return (parent_flags, parent_flags * keep_flags)


def draw_parent_blocks(key, part):
    return structure_flags(key)[0]


def draw_child_blocks(key, part):
    return structure_flags(key)[1]


def spiked(drawn, stream_key, source, target, parts, factor):
    owner, partner = [(jnp.arange(drawn.shape[position]) // (drawn.shape[position] // parts)).reshape([-1 if axis == position else 1 for axis in range(drawn.ndim)]) for position in (source, target)]
    chosen = jax.random.permutation(stream_key, parts)[partner]
    strong = (owner == chosen) | (owner == (partner + parts // 2) % parts)
    return jnp.where(strong, factor * drawn, drawn)


def level_of(own_key, shape, pieces, smallest, high):
    def one(axis_at, parts):
        steps = jax.random.uniform(jax.random.fold_in(jax.random.fold_in(own_key, 6), axis_at), (parts,), jnp.float32, smallest / len(pieces), high / len(pieces))
        return jnp.repeat(jnp.exp(steps), shape[axis_at] // parts).reshape((-1,) + (1,) * (len(shape) - axis_at - 1))

    level = one(*pieces[0])
    for cut in pieces[1:]:
        level = level * one(*cut)
    return level


def bell_draw(stream_key, shape, spread, limit, pieces=(), dtype=jnp.bfloat16):
    factor_of = level_of(stream_key, shape, pieces, -0.22, 0.18) if pieces else 1.0
    entries = jax.random.normal(stream_key, shape, jnp.float32) * spread * factor_of
    return jnp.minimum(jnp.maximum(entries, -limit), limit).astype(dtype)


def noise_with(own_key, dims, scale, reach, cuts, heavy, kind=jnp.bfloat16):
    result = scale * jax.random.normal(own_key, dims, jnp.float32)
    if cuts:
        result = result * level_of(own_key, dims, cuts, -0.22, 0.18)
    return jnp.clip(spiked(result, jax.random.fold_in(own_key, 3), *heavy), -reach, reach).astype(kind)


def setup_inputs(seed: int = 0) -> dict:
    key_of = jax.random.split(jax.random.key(seed), 9)
    inverse = noise_with(key_of[0], (M, M), M ** -0.5, 0.0546875, ((0, 8), (1, 16)), (1, 0, 16, 2.0), jnp.float32)
    parent_panel = bell_draw(key_of[1], (M, W), 0.3, 1.8, ((0, 128),), jnp.float32)
    child_panel = bell_draw(key_of[2], (M, W), 0.3, 1.8, ((0, 128),), jnp.float32)
    child_top = bell_draw(key_of[3], (W, W), W ** -0.5, 0.375, (), jnp.float32)
    diag_parent = bell_draw(key_of[4], (W, W), 2.0, 12.0, (), jnp.float32)
    diag_child = bell_draw(key_of[5], (W, W), 2.0, 12.0, (), jnp.float32)
    parent_blocks = draw_parent_blocks(jax.random.fold_in(key_of[8], 71), 0)
    child_blocks = draw_child_blocks(jax.random.fold_in(key_of[8], 71), 0)
    return dict(inverse=inverse, parent_panel=parent_panel, child_panel=child_panel, child_top=child_top, diag_parent=diag_parent, diag_child=diag_child, parent_blocks=parent_blocks, child_blocks=child_blocks)


def expand_mask(blocks):
    flags = jnp.repeat(blocks, BLK, total_repeat_length=blocks.shape[0] * BLK)
    return flags.astype(jnp.float32)[:, None]


def matmul(left, right):
    return jnp.dot(left, right, precision=lax.Precision.HIGHEST, preferred_element_type=jnp.float32)


def reference(inverse, parent_panel, child_panel, child_top, diag_parent, diag_child, parent_blocks, child_blocks):
    parent_mask = expand_mask(parent_blocks)
    child_mask = expand_mask(child_blocks)
    parent_masked = parent_panel * parent_mask
    child_masked = child_panel * child_mask
    parent_image = matmul(inverse, parent_masked)
    child_image = matmul(inverse, child_masked)
    parent_column = -(parent_mask * parent_image)
    parent_diagonal = diag_parent - matmul(parent_masked.T, parent_column)
    child_column = -(child_mask * (matmul(parent_column, child_top) + child_image))
    child_upper = -(matmul(parent_diagonal, child_top) + matmul(parent_column.T, child_masked))
    child_diagonal = diag_child - matmul(child_top.T, child_upper) - matmul(child_masked.T, child_column)
    return parent_column, parent_diagonal, child_column, child_upper, child_diagonal
```

```python
import jax
import jax.numpy as jnp
from jax import lax
from jax.sharding import Mesh, PartitionSpec as P

BLK = 128
AXES = ("y", "zh", "zl", "x", "c")
RING_UP = [(i, (i + 1) % 4) for i in range(4)]
RING_DOWN = [(i, (i + 3) % 4) for i in range(4)]
SWAP = [(0, 1), (1, 0)]


def flip(bits, size):
    return [(i, i ^ bits) for i in range(size)]


def matmul(left, right):
    return jnp.dot(left, right, precision=lax.Precision.HIGH, preferred_element_type=jnp.float32)


def spread_pairs():
    pairs = []
    for source in range(128):
        y, zh, zl, x, c = source >> 5, source >> 4 & 1, source >> 3 & 1, source >> 1 & 3, source & 1
        target = ((x + y) % 4, c, y >> 1, (y & 1) * 2 + zh, zl)
        pairs.append((source, ((((target[0] * 2 + target[1]) * 2 + target[2]) * 4 + target[3]) * 2 + target[4])))
    return pairs


def gather_rows(piece, zh, shift):
    width = piece.shape[1]
    spread = lax.ppermute(piece, AXES, spread_pairs())
    other = lax.ppermute(spread, "zh", SWAP)
    pair = jnp.where(zh == 0, jnp.concatenate([spread, other]), jnp.concatenate([other, spread]))
    up = lax.ppermute(pair, "y", RING_UP)
    down = lax.ppermute(pair, "y", RING_DOWN)
    half = piece.shape[0]
    far_low = lax.ppermute(up[:half], "y", RING_UP)
    far_high = lax.ppermute(down[half:], "y", RING_DOWN)
    rows = jnp.stack([pair, down, jnp.concatenate([far_low, far_high]), up])
    return jnp.roll(rows, shift, axis=0).reshape(8 * half, width)


def scatter_sum(partial, zl, x, c):
    rows = partial.shape[0] // 16
    width = partial.shape[1]
    parts = partial.reshape(2, 4, 2, rows, width)
    take = lambda array, index, axis: lax.dynamic_index_in_dim(array, index, axis, keepdims=False)
    own = take(parts, c, 2) + lax.ppermute(take(parts, 1 - c, 2), "c", SWAP)
    at = [take(own, (x + step) % 4, 1) for step in range(4)]
    half = rows // 2
    low = lax.ppermute(at[2][:, :half], "x", RING_UP)
    high = lax.ppermute(at[2][:, half:], "x", RING_DOWN)
    up = jnp.concatenate([at[1][:, :half] + low, at[1][:, half:]], axis=1)
    down = jnp.concatenate([at[3][:, :half], at[3][:, half:] + high], axis=1)
    total = at[0] + lax.ppermute(up, "x", RING_UP) + lax.ppermute(down, "x", RING_DOWN)
    return take(total, zl, 0) + lax.ppermute(take(total, 1 - zl, 0), "zl", SWAP)


def sum_all(local, x, c):
    rows, width = local.shape
    take = lambda array, index: lax.dynamic_index_in_dim(array, index, 0, keepdims=False)
    cores = local.reshape(2, rows // 2, width)
    own = take(cores, c) + lax.ppermute(take(cores, 1 - c), "c", SWAP)
    quarters = own.reshape(4, rows // 8, width)
    got = [lax.ppermute(take(quarters, x ^ bits), "x", flip(bits, 4)) for bits in (1, 2, 3)]
    own = (take(quarters, x) + got[0]) + (got[1] + got[2])
    got = [lax.ppermute(own, "y", flip(bits, 4)) for bits in (1, 2, 3)]
    own = (own + got[0]) + (got[1] + got[2])
    got = [lax.ppermute(own, ("zh", "zl"), flip(bits, 4)) for bits in (1, 2, 3)]
    own = (own + got[0]) + (got[1] + got[2])
    got = [own] + [lax.ppermute(own, "x", flip(bits, 4)) for bits in (1, 2, 3)]
    stacked = jnp.stack(got)
    order = [take(stacked, x ^ bits) for bits in range(4)]
    own = jnp.concatenate(order)
    other = lax.ppermute(own, "c", SWAP)
    return jnp.where(c == 0, jnp.concatenate([own, other]), jnp.concatenate([other, own]))


def local_mask(blocks, device, rows):
    step = 64
    flags = jnp.repeat(blocks, BLK // step, total_repeat_length=blocks.shape[0] * (BLK // step))
    own = lax.dynamic_slice_in_dim(flags, device * (rows // step), rows // step)
    return jnp.repeat(own, step, total_repeat_length=rows).astype(jnp.float32)[:, None]


def device_step(inverse, parent_panel, child_panel, child_top, diag_parent, diag_child, parent_blocks, child_blocks):
    y, zh, zl, x, c = [lax.axis_index(name) for name in AXES]
    device = (((y * 2 + zh) * 2 + zl) * 4 + x) * 2 + c
    rows = parent_panel.shape[0]
    parent_mask = local_mask(parent_blocks, device, rows)
    child_mask = local_mask(child_blocks, device, rows)
    parent_masked = parent_panel * parent_mask
    child_masked = child_panel * child_mask
    shift = (y - (zl * 2 + x // 2)) % 4
    parent_rows = gather_rows(parent_masked, zh, shift)
    child_rows = gather_rows(child_masked, zh, shift)
    parent_image = scatter_sum(matmul(inverse, parent_rows), zl, x, c)
    child_image = scatter_sum(matmul(inverse, child_rows), zl, x, c)
    parent_column = -(parent_mask * parent_image)
    child_column = -(child_mask * (matmul(parent_column, child_top) + child_image))
    products = sum_all(
        jnp.concatenate(
            [
                matmul(parent_masked.T, parent_column),
                matmul(parent_column.T, child_masked),
                matmul(child_masked.T, child_column),
            ]
        ),
        x,
        c,
    )
    width = parent_panel.shape[1]
    parent_diagonal = diag_parent - products[:width]
    child_upper = -(matmul(parent_diagonal, child_top) + products[width : 2 * width])
    child_diagonal = diag_child - matmul(child_top.T, child_upper) - products[2 * width :]
    return parent_column, parent_diagonal, child_column, child_upper, child_diagonal


def solution(mesh):
    fine = Mesh(mesh.devices.reshape(4, 2, 2, 4, 2), AXES)
    everywhere = P(AXES, None)
    whole = P(None, None)
    return jax.shard_map(
        device_step,
        mesh=fine,
        in_specs=(P(("y", "zh"), ("zl", "x", "c")), everywhere, everywhere, whole, whole, whole, P(None), P(None)),
        out_specs=(everywhere, whole, everywhere, whole, whole),
        check_vma=False,
    )
```

```python
import jax
import jax.numpy as jnp
from jax import lax
from jax.experimental import pallas as pl
from jax.experimental.pallas import tpu as pltpu
from jax.sharding import Mesh, PartitionSpec as P

BLK = 128
AXES = ("y", "zh", "zl", "x", "c")
RING_UP = [(i, (i + 1) % 4) for i in range(4)]
RING_DOWN = [(i, (i + 3) % 4) for i in range(4)]
SWAP = [(0, 1), (1, 0)]


def flip(bits, size):
    return [(i, i ^ bits) for i in range(size)]


def matmul(left, right):
    return jnp.dot(left, right, precision=lax.Precision.HIGH, preferred_element_type=jnp.float32)


def spread_pairs():
    pairs = []
    for source in range(128):
        y, zh, zl, x, c = source >> 5, source >> 4 & 1, source >> 3 & 1, source >> 1 & 3, source & 1
        target = ((x + y) % 4, c, y >> 1, (y & 1) * 2 + zh, zl)
        pairs.append((source, ((((target[0] * 2 + target[1]) * 2 + target[2]) * 4 + target[3]) * 2 + target[4])))
    return pairs


def split(value):
    high = value.astype(jnp.bfloat16)
    return high, (value - high.astype(jnp.float32)).astype(jnp.bfloat16)


def product_kernel(other_core, inverse, rows, out, right_high, right_low, buffers, sems):
    y, _, zl, x, c = [lax.axis_index(name) for name in AXES]
    core = 1 - c if other_core else c
    chunks, size, _ = out.shape
    steps = chunks // 2
    slots = buffers.shape[0]

    def copies(t):
        slot = t % slots
        starts = [pl.multiple_of(((zl ^ side) * 8 + (x + t) % 4 * 2 + core) * size, 64) for side in range(2)]
        return [
            pltpu.make_async_copy(
                inverse.at[pl.ds(start, size)], buffers.at[slot, pl.ds(side * size, size)], sems.at[slot, side]
            )
            for side, start in enumerate(starts)
        ]

    for t in range(slots):
        for copy in copies(t):
            copy.start()

    shift = (y - (zl * 2 + x // 2) + 4) % 4
    group_rows = rows.shape[0] // 4
    for offset in range(4):
        start = pl.multiple_of((offset + shift) % 4 * group_rows, BLK)
        high, low = split(rows[offset * group_rows : (offset + 1) * group_rows, :])
        right_high[pl.ds(start, group_rows), :] = high
        right_low[pl.ds(start, group_rows), :] = low

    def step(t, carry):
        for copy in copies(t):
            copy.wait()
        high, low = split(buffers[t % slots])
        dot = lambda a, b: jnp.dot(a, b, preferred_element_type=jnp.float32)
        total = dot(high, right_high[...]) + (dot(high, right_low[...]) + dot(low, right_high[...]))
        out[2 * t] = total[:size]
        out[2 * t + 1] = total[size:]

        @pl.when(t + slots < steps)
        def _():
            for copy in copies(t + slots):
                copy.start()

        return carry

    lax.fori_loop(0, steps, step, 0)


def block_product(inverse, rows, other_core):
    size = inverse.shape[0] // 16
    width = rows.shape[1]
    slots = 3
    whole = pl.BlockSpec(memory_space=pltpu.VMEM)
    return pl.pallas_call(
        lambda *refs: product_kernel(other_core, *refs),
        out_shape=jax.ShapeDtypeStruct((8, size, width), jnp.float32),
        in_specs=[pl.BlockSpec(memory_space=pltpu.HBM), whole],
        out_specs=whole,
        scratch_shapes=[
            pltpu.VMEM(rows.shape, jnp.bfloat16),
            pltpu.VMEM(rows.shape, jnp.bfloat16),
            pltpu.VMEM((slots, 2 * size, inverse.shape[1]), jnp.float32),
            pltpu.SemaphoreType.DMA((slots, 2)),
        ],
        compiler_params=pltpu.CompilerParams(vmem_limit_bytes=46 * 1024 * 1024),
        cost_estimate=pl.CostEstimate(flops=6 * size * 8 * inverse.shape[1] * width, bytes_accessed=inverse.size * 2, transcendentals=0),
        name="send_product" if other_core else "keep_product",
    )(inverse, rows)


def combine_kernel(keep, got, own_rows, zl_rows, down_rows, low_rows, high_rows, up_rows,
                   mine, far_low, far_high, near_up, near_down, products, sums):
    x, c = lax.axis_index("x"), lax.axis_index("c")
    _, size, both = keep.shape
    width = both // 2
    half = size // 2
    sums[...] = jnp.zeros_like(sums)

    def chunk(offset, side):
        total = keep[2 * offset + side] + got[2 * offset + side]
        if offset == 0:
            rows = (own_rows, zl_rows)[side][...]
            mine[side] = total
        elif offset == 1:
            rows = down_rows[side]
            near_up[side] = total
        elif offset == 2:
            rows = (low_rows, high_rows)[side][...]
            far_low[side] = total[:half]
            far_high[side] = total[half:]
        else:
            rows = up_rows[side]
            near_down[side] = total
        return total, rows

    for offset in range(4):
        totals, rows = zip(*[chunk(offset, side) for side in range(2)])
        image_high, image_low = split(jnp.concatenate(totals))
        rows_high, rows_low = split(jnp.concatenate(rows))
        across = (((0,), (0,)), ((), ()))
        dot = lambda a, b: lax.dot_general(a, b, across, preferred_element_type=jnp.float32)
        product = lambda ah, al, bh, bl: dot(ah, bh) + (dot(ah, bl) + dot(al, bh))
        sums[: 2 * width] += product(rows_high, rows_low, image_high[:, :width], image_low[:, :width])
        sums[2 * width :] += product(
            rows_high[:, width:], rows_low[:, width:], image_high[:, width:], image_low[:, width:]
        )
    part = sums.shape[0] // 8
    for dc in range(2):
        for dx in range(4):
            start = pl.multiple_of(((c ^ dc) * 4 + (x ^ dx)) * part, 8)
            products[dc, dx] = sums[pl.ds(start, part), :]


def combine(keep, got, pieces):
    _, size, both = keep.shape
    width = both // 2
    part = jax.ShapeDtypeStruct((2, size, both), jnp.float32)
    half = jax.ShapeDtypeStruct((2, size // 2, both), jnp.float32)
    products = jax.ShapeDtypeStruct((2, 4, 3 * width // 8, width), jnp.float32)
    whole = pl.BlockSpec(memory_space=pltpu.VMEM)
    return pl.pallas_call(
        combine_kernel,
        out_shape=(part, half, half, part, part, products),
        in_specs=[whole] * 8,
        out_specs=[whole] * 6,
        scratch_shapes=[pltpu.VMEM((3 * width, width), jnp.float32)],
        compiler_params=pltpu.CompilerParams(vmem_limit_bytes=24 * 1024 * 1024),
        cost_estimate=pl.CostEstimate(flops=18 * 8 * size * width * width, bytes_accessed=keep.size * 16, transcendentals=0),
        name="combine",
    )(keep, got, *pieces)


def finish_kernel(own, other, child_top, diag_parent, diag_child, parent_diagonal, child_upper, child_diagonal, sums):
    x, c = lax.axis_index("x"), lax.axis_index("c")
    part = own.shape[1]
    width = child_top.shape[0]
    for dc, source in enumerate((own, other)):
        for dx in range(4):
            start = pl.multiple_of(((c ^ dc) * 4 + (x ^ dx)) * part, 8)
            sums[pl.ds(start, part), :] = source[dx]

    def dot(a, b, dims=(((1,), (0,)), ((), ()))):
        return lax.dot_general(a, b, dims, precision=lax.Precision.HIGHEST, preferred_element_type=jnp.float32)

    top = child_top[...]
    cross = sums[width : 2 * width]
    diagonal = diag_parent[...] + sums[:width]
    parent_diagonal[...] = diagonal
    upper = cross.T - dot(diagonal, top)
    child_upper[...] = upper
    inner = dot(top, upper, (((0,), (0,)), ((), ()))) + dot(cross, top)
    child_diagonal[...] = diag_child[...] - inner + sums[2 * width :]


def finish(own, other, child_top, diag_parent, diag_child):
    whole = pl.BlockSpec(memory_space=pltpu.VMEM)
    block = jax.ShapeDtypeStruct(child_top.shape, jnp.float32)
    return pl.pallas_call(
        finish_kernel,
        out_shape=(block, block, block),
        in_specs=[whole] * 5,
        out_specs=[whole] * 3,
        scratch_shapes=[pltpu.VMEM((3 * child_top.shape[0], child_top.shape[1]), jnp.float32)],
        compiler_params=pltpu.CompilerParams(vmem_limit_bytes=16 * 1024 * 1024),
        name="finish",
    )(own, other, child_top, diag_parent, diag_child)


def sum_all(products):
    own = products[0] + lax.ppermute(products[1], "c", SWAP)
    got = [lax.ppermute(own[bits], "x", flip(bits, 4)) for bits in (1, 2, 3)]
    own = (own[0] + got[0]) + (got[1] + got[2])
    got = [lax.ppermute(own, "y", flip(bits, 4)) for bits in (1, 2, 3)]
    own = (own + got[0]) + (got[1] + got[2])
    got = [lax.ppermute(own, ("zh", "zl"), flip(bits, 4)) for bits in (1, 2, 3)]
    own = (own + got[0]) + (got[1] + got[2])
    own = jnp.stack([own] + [lax.ppermute(own, "x", flip(bits, 4)) for bits in (1, 2, 3)])
    return own, lax.ppermute(own, "c", SWAP)


def images_of(masked, inverse, zh):
    rows, _ = masked.shape
    spread = lax.ppermute(masked, AXES, spread_pairs())
    other = lax.ppermute(spread, "zh", SWAP)
    pair = jnp.where(zh == 0, jnp.concatenate([spread, other]), jnp.concatenate([other, spread]))
    up = lax.ppermute(pair, "y", RING_UP)
    down = lax.ppermute(pair, "y", RING_DOWN)
    low = lax.ppermute(up[:rows], "y", RING_UP)
    high = lax.ppermute(down[rows:], "y", RING_DOWN)
    gathered = jnp.concatenate([pair, down, low, high, up])
    row_side = lax.ppermute(masked, "zl", SWAP)
    row_pair = jnp.stack([masked, row_side])
    row_up = lax.ppermute(row_pair, "x", RING_UP)
    row_down = lax.ppermute(row_pair, "x", RING_DOWN)
    row_low = lax.ppermute(row_up[0], "x", RING_UP)
    row_high = lax.ppermute(row_down[1], "x", RING_DOWN)
    send = block_product(inverse, gathered, True)
    keep = block_product(inverse, gathered, False)
    got = lax.ppermute(send, "c", SWAP)
    mine, far_low, far_high, near_up, near_down, products = combine(
        keep, got, (masked, row_side, row_down, row_low, row_high, row_up)
    )
    half = rows // 2
    far_low = lax.ppermute(far_low, "x", RING_UP)
    far_high = lax.ppermute(far_high, "x", RING_DOWN)
    from_low = jnp.concatenate([near_up[:, :half] + far_low, near_up[:, half:]], axis=1)
    from_high = jnp.concatenate([near_down[:, :half], near_down[:, half:] + far_high], axis=1)
    from_low = lax.ppermute(from_low, "x", RING_UP)
    from_high = lax.ppermute(from_high, "x", RING_DOWN)
    last = lax.ppermute(mine[1] + from_low[1] + from_high[1], "zl", SWAP)
    return mine[0] + from_low[0] + from_high[0] + last, products


def local_mask(blocks, device, rows):
    block = (device * rows + lax.broadcasted_iota(jnp.int32, (rows, blocks.shape[0]), 0)) // BLK
    chosen = block == lax.broadcasted_iota(jnp.int32, (rows, blocks.shape[0]), 1)
    return jnp.sum(jnp.where(chosen, blocks[None, :].astype(jnp.float32), 0.0), axis=1, keepdims=True)


def local_step(inverse, parent_panel, child_panel, child_top, diag_parent, diag_child, parent_blocks, child_blocks):
    y, zh, zl, x, c = [lax.axis_index(name) for name in AXES]
    device = (((y * 2 + zh) * 2 + zl) * 4 + x) * 2 + c
    rows = parent_panel.shape[0]
    parent_mask = local_mask(parent_blocks, device, rows)
    child_mask = local_mask(child_blocks, device, rows)
    masked = jnp.concatenate([parent_panel * parent_mask, child_panel * child_mask], axis=1)
    images, products = images_of(masked, inverse, zh)
    width = parent_panel.shape[1]
    parent_column = -(parent_mask * images[:, :width])
    child_column = -(child_mask * (matmul(parent_column, child_top) + images[:, width:]))
    parent_diagonal, child_upper, child_diagonal = finish(*sum_all(products), child_top, diag_parent, diag_child)
    return parent_column, parent_diagonal, child_column, child_upper, child_diagonal


def solution(mesh):
    fine = Mesh(mesh.devices.reshape(4, 2, 2, 4, 2), AXES)
    everywhere = P(AXES, None)
    whole = P(None, None)
    return jax.shard_map(
        local_step,
        mesh=fine,
        in_specs=(P(("y", "zh"), ("zl", "x", "c")), everywhere, everywhere, whole, whole, whole, P(None), P(None)),
        out_specs=(everywhere, whole, everywhere, whole, whole),
        check_vma=False,
    )
```

```python
import jax
import jax.numpy as jnp
from jax import lax
from jax.experimental import pallas as pl
from jax.experimental.pallas import tpu as pltpu
from jax.sharding import Mesh, PartitionSpec as P

BLK = 128
AXES = ("y", "zh", "zl", "x", "c")
RING_UP = [(i, (i + 1) % 4) for i in range(4)]
RING_DOWN = [(i, (i + 3) % 4) for i in range(4)]
SWAP = [(0, 1), (1, 0)]


def flip(bits, size):
    return [(i, i ^ bits) for i in range(size)]


def spread_pairs():
    pairs = []
    for source in range(128):
        y, zh, zl, x, c = source >> 5, source >> 4 & 1, source >> 3 & 1, source >> 1 & 3, source & 1
        target = ((x + y) % 4, c, y >> 1, (y & 1) * 2 + zh, zl)
        pairs.append((source, ((((target[0] * 2 + target[1]) * 2 + target[2]) * 4 + target[3]) * 2 + target[4])))
    return pairs


def split(value):
    high = value.astype(jnp.bfloat16)
    return high, (value - high.astype(jnp.float32)).astype(jnp.bfloat16)


def product_kernel(offsets, cores, carried, inverse, *refs):
    pieces, refs = refs[: len(offsets)], refs[len(offsets) :]
    prior = refs[0] if carried else None
    out, right_high, right_low, buffers, sems = refs[1 if carried else 0 :]
    y, _, zl, x, c = [lax.axis_index(name) for name in AXES]
    _, chunks, size, _ = out.shape
    group = pieces[0].shape[0]
    shift = (y - (zl * 2 + x // 2) + 4) % 4
    slots = buffers.shape[0]
    half = chunks // 2
    steps = len(cores) * half

    def copies(u):
        slot = u % slots
        core = (c + 1 - u // half) % 2 if len(cores) == 2 else (c + 1 - cores[0]) % 2
        found = []
        for side in range(2):
            start = pl.multiple_of(((zl ^ side) * 8 + (x + u % half) % 4 * 2 + core) * size, 64)
            for place, offset in enumerate(offsets):
                column = pl.multiple_of((offset + shift) % 4 * group, BLK)
                found.append(
                    pltpu.make_async_copy(
                        inverse.at[pl.ds(start, size), pl.ds(column, group)],
                        buffers.at[slot, pl.ds(side * size, size), pl.ds(place * group, group)],
                        sems.at[slot, side * len(offsets) + place],
                    )
                )
        return found

    for u in range(slots):
        for copy in copies(u):
            copy.start()
    for place, piece in enumerate(pieces):
        high, low = split(piece[...])
        right_high[place * group : (place + 1) * group, :] = high
        right_low[place * group : (place + 1) * group, :] = low

    def step(u, carry):
        for copy in copies(u):
            copy.wait()
        high, low = split(buffers[u % slots])
        dot = lambda a, b: jnp.dot(a, b, preferred_element_type=jnp.float32)
        total = dot(high, right_high[...]) + (dot(high, right_low[...]) + dot(low, right_high[...]))
        place = u // half
        for side in range(2):
            part = total[side * size : (side + 1) * size]
            if carried:
                part = part + prior[place if len(cores) == 2 else cores[0], 2 * (u % half) + side]
            out[place, 2 * (u % half) + side] = part

        @pl.when(u + slots < steps)
        def _():
            for copy in copies(u + slots):
                copy.start()

        return carry

    lax.fori_loop(0, steps, step, 0)


def block_product(inverse, offsets, cores, pieces, prior=None):
    size = inverse.shape[0] // 16
    group, width = pieces[0].shape
    slots = 3
    depth = group * len(offsets)
    whole = pl.BlockSpec(memory_space=pltpu.VMEM)
    carried = prior is not None
    operands = list(pieces) + ([prior] if carried else [])
    return pl.pallas_call(
        lambda *refs: product_kernel(offsets, cores, carried, *refs),
        out_shape=jax.ShapeDtypeStruct((len(cores), 8, size, width), jnp.float32),
        in_specs=[pl.BlockSpec(memory_space=pltpu.HBM)] + [whole] * len(operands),
        out_specs=whole,
        scratch_shapes=[
            pltpu.VMEM((depth, width), jnp.bfloat16),
            pltpu.VMEM((depth, width), jnp.bfloat16),
            pltpu.VMEM((slots, 2 * size, depth), jnp.float32),
            pltpu.SemaphoreType.DMA((slots, 2 * len(offsets))),
        ],
        compiler_params=pltpu.CompilerParams(vmem_limit_bytes=32 * 1024 * 1024),
        cost_estimate=pl.CostEstimate(
            flops=6 * size * 8 * len(cores) * depth * width, bytes_accessed=size * 8 * len(cores) * depth * 4, transcendentals=0
        ),
        name="product",
    )(inverse, *operands)


def row_masks(device, rows, parent_flags, child_flags):
    block = device * rows // BLK
    border = (block + 1) * BLK - device * rows
    row = lax.broadcasted_iota(jnp.int32, (rows, 1), 0)
    pick = lambda flags: jnp.where(row < border, flags[block], flags[block + 1]).astype(jnp.float32)
    return pick(parent_flags), pick(child_flags)


def device_index():
    y, zh, zl, x, c = [lax.axis_index(name) for name in AXES]
    return (((y * 2 + zh) * 2 + zl) * 4 + x) * 2 + c


def mask_kernel(parent_flags, child_flags, parent_panel, child_panel, masked, sems):
    rows, width = parent_panel.shape
    halves = [masked.at[:, pl.ds(place * width, width)] for place in range(2)]
    copies = [
        pltpu.make_async_copy(panel, half, sems.at[place])
        for place, (panel, half) in enumerate(zip((parent_panel, child_panel), halves))
    ]
    for copy in copies:
        copy.start()
    for mask, copy, half in zip(row_masks(device_index(), rows, parent_flags, child_flags), copies, halves):
        copy.wait()
        half[...] = mask * half[...]


def mask_panels(parent_flags, child_flags, parent_panel, child_panel):
    rows, width = parent_panel.shape
    far = pl.BlockSpec(memory_space=pltpu.HBM)
    scalars = pl.BlockSpec(memory_space=pltpu.SMEM)
    return pl.pallas_call(
        mask_kernel,
        out_shape=jax.ShapeDtypeStruct((rows, 2 * width), jnp.float32),
        in_specs=[scalars, scalars, far, far],
        out_specs=pl.BlockSpec(memory_space=pltpu.VMEM),
        scratch_shapes=[pltpu.SemaphoreType.DMA((2,))],
        compiler_params=pltpu.CompilerParams(vmem_limit_bytes=62_900_000),
        name="mask_panels",
    )(parent_flags, child_flags, parent_panel, child_panel)


def columns_kernel(parent_flags, child_flags, mine, from_low, from_high, last, child_top, parent_column, child_column):
    rows, width = parent_column.shape
    parent_mask, child_mask = row_masks(device_index(), rows, parent_flags, child_flags)
    image = mine[0] + from_low[0] + from_high[0] + last[...]
    column = -(parent_mask * image[:, :width])
    parent_column[...] = column
    across = jnp.dot(column, child_top[...], precision=lax.Precision.HIGHEST, preferred_element_type=jnp.float32)
    child_column[...] = -(child_mask * (across + image[:, width:]))


def columns(parent_flags, child_flags, parts, child_top):
    rows, both = parts[-1].shape
    whole = pl.BlockSpec(memory_space=pltpu.VMEM)
    scalars = pl.BlockSpec(memory_space=pltpu.SMEM)
    block = jax.ShapeDtypeStruct((rows, both // 2), jnp.float32)
    return pl.pallas_call(
        columns_kernel,
        out_shape=(block, block),
        in_specs=[scalars, scalars] + [whole] * 5,
        out_specs=[whole, whole],
        compiler_params=pltpu.CompilerParams(vmem_limit_bytes=16 * 1024 * 1024),
        name="columns",
    )(parent_flags, child_flags, *parts, child_top)


def combine_kernel(keep, got, own_rows, zl_rows, down_rows, low_rows, high_rows, up_rows,
                   mine, far_low, far_high, near_up, near_down, products, sums):
    x, c = lax.axis_index("x"), lax.axis_index("c")
    _, _, size, both = keep.shape
    width = both // 2
    half = size // 2
    sums[...] = jnp.zeros_like(sums)

    def chunk(offset, side):
        total = keep[0, 2 * offset + side] + got[0, 2 * offset + side]
        if offset == 0:
            rows = (own_rows, zl_rows)[side][...]
            mine[side] = total
        elif offset == 1:
            rows = down_rows[side]
            near_up[side] = total
        elif offset == 2:
            rows = (low_rows, high_rows)[side][...]
            far_low[side] = total[:half]
            far_high[side] = total[half:]
        else:
            rows = up_rows[side]
            near_down[side] = total
        return total, rows

    for offset in range(4):
        totals, rows = zip(*[chunk(offset, side) for side in range(2)])
        image_high, image_low = split(jnp.concatenate(totals))
        rows_high, rows_low = split(jnp.concatenate(rows))
        across = (((0,), (0,)), ((), ()))
        dot = lambda a, b: lax.dot_general(a, b, across, preferred_element_type=jnp.float32)
        product = lambda ah, al, bh, bl: dot(ah, bh) + (dot(ah, bl) + dot(al, bh))
        sums[: 2 * width] += product(rows_high, rows_low, image_high[:, :width], image_low[:, :width])
        sums[2 * width :] += product(
            rows_high[:, width:], rows_low[:, width:], image_high[:, width:], image_low[:, width:]
        )
    part = sums.shape[0] // 8
    for dc in range(2):
        for dx in range(4):
            start = pl.multiple_of(((c ^ dc) * 4 + (x ^ dx)) * part, 8)
            products[dc, dx] = sums[pl.ds(start, part), :]


def combine(keep, got, pieces):
    _, _, size, both = keep.shape
    width = both // 2
    part = jax.ShapeDtypeStruct((2, size, both), jnp.float32)
    half = jax.ShapeDtypeStruct((2, size // 2, both), jnp.float32)
    products = jax.ShapeDtypeStruct((2, 4, 3 * width // 8, width), jnp.float32)
    whole = pl.BlockSpec(memory_space=pltpu.VMEM)
    return pl.pallas_call(
        combine_kernel,
        out_shape=(part, half, half, part, part, products),
        in_specs=[whole] * 8,
        out_specs=[whole] * 6,
        scratch_shapes=[pltpu.VMEM((3 * width, width), jnp.float32)],
        compiler_params=pltpu.CompilerParams(vmem_limit_bytes=24 * 1024 * 1024),
        cost_estimate=pl.CostEstimate(flops=18 * 8 * size * width * width, bytes_accessed=keep.size * 16, transcendentals=0),
        name="combine",
    )(keep, got, *pieces)


def finish_kernel(own, other, child_top, diag_parent, diag_child, parent_diagonal, child_upper, child_diagonal, sums):
    x, c = lax.axis_index("x"), lax.axis_index("c")
    part = own.shape[1]
    width = child_top.shape[0]
    for dc, source in enumerate((own, other)):
        for dx in range(4):
            start = pl.multiple_of(((c ^ dc) * 4 + (x ^ dx)) * part, 8)
            sums[pl.ds(start, part), :] = source[dx]

    def dot(a, b, dims=(((1,), (0,)), ((), ()))):
        return lax.dot_general(a, b, dims, precision=lax.Precision.HIGHEST, preferred_element_type=jnp.float32)

    top = child_top[...]
    cross = sums[width : 2 * width]
    diagonal = diag_parent[...] + sums[:width]
    parent_diagonal[...] = diagonal
    upper = cross.T - dot(diagonal, top)
    child_upper[...] = upper
    inner = dot(top, upper, (((0,), (0,)), ((), ()))) + dot(cross, top)
    child_diagonal[...] = diag_child[...] - inner + sums[2 * width :]


def finish(own, other, child_top, diag_parent, diag_child):
    whole = pl.BlockSpec(memory_space=pltpu.VMEM)
    block = jax.ShapeDtypeStruct(child_top.shape, jnp.float32)
    return pl.pallas_call(
        finish_kernel,
        out_shape=(block, block, block),
        in_specs=[whole] * 5,
        out_specs=[whole] * 3,
        scratch_shapes=[pltpu.VMEM((3 * child_top.shape[0], child_top.shape[1]), jnp.float32)],
        compiler_params=pltpu.CompilerParams(vmem_limit_bytes=16 * 1024 * 1024),
        name="finish",
    )(own, other, child_top, diag_parent, diag_child)


def sum_all(products):
    own = products[0] + lax.ppermute(products[1], "c", SWAP)
    got = [lax.ppermute(own[bits], "x", flip(bits, 4)) for bits in (1, 2, 3)]
    own = (own[0] + got[0]) + (got[1] + got[2])
    got = [lax.ppermute(own, "y", flip(bits, 4)) for bits in (1, 2, 3)]
    own = (own + got[0]) + (got[1] + got[2])
    got = [lax.ppermute(own, ("zh", "zl"), flip(bits, 4)) for bits in (1, 2, 3)]
    own = (own + got[0]) + (got[1] + got[2])
    own = jnp.stack([own] + [lax.ppermute(own, "x", flip(bits, 4)) for bits in (1, 2, 3)])
    return own, lax.ppermute(own, "c", SWAP)


def images_of(masked, inverse, zh):
    rows, _ = masked.shape
    spread = lax.ppermute(masked, AXES, spread_pairs())
    other = lax.ppermute(spread, "zh", SWAP)
    pair = jnp.where(zh == 0, jnp.concatenate([spread, other]), jnp.concatenate([other, spread]))
    up = lax.ppermute(pair, "y", RING_UP)
    down = lax.ppermute(pair, "y", RING_DOWN)
    low = lax.ppermute(up[:rows], "y", RING_UP)
    high = lax.ppermute(down[rows:], "y", RING_DOWN)
    row_side = lax.ppermute(masked, "zl", SWAP)
    row_pair = jnp.stack([masked, row_side])
    row_up = lax.ppermute(row_pair, "x", RING_UP)
    row_down = lax.ppermute(row_pair, "x", RING_DOWN)
    row_low = lax.ppermute(row_up[0], "x", RING_UP)
    row_high = lax.ppermute(row_down[1], "x", RING_DOWN)
    total = block_product(inverse, (0,), (0, 1), [pair])
    total = block_product(inverse, (1, 3), (0, 1), [down, up], total)
    far = jnp.concatenate([low, high])
    send = block_product(inverse, (2,), (0,), [far], total)
    keep = block_product(inverse, (2,), (1,), [far], total)
    got = lax.ppermute(send, "c", SWAP)
    mine, far_low, far_high, near_up, near_down, products = combine(
        keep, got, (masked, row_side, row_down, row_low, row_high, row_up)
    )
    half = rows // 2
    far_low = lax.ppermute(far_low, "x", RING_UP)
    far_high = lax.ppermute(far_high, "x", RING_DOWN)
    from_low = jnp.concatenate([near_up[:, :half] + far_low, near_up[:, half:]], axis=1)
    from_high = jnp.concatenate([near_down[:, :half], near_down[:, half:] + far_high], axis=1)
    from_low = lax.ppermute(from_low, "x", RING_UP)
    from_high = lax.ppermute(from_high, "x", RING_DOWN)
    last = lax.ppermute(mine[1] + from_low[1] + from_high[1], "zl", SWAP)
    return (mine, from_low, from_high, last), products


def local_step(inverse, parent_panel, child_panel, child_top, diag_parent, diag_child, parent_blocks, child_blocks):
    masked = mask_panels(parent_blocks, child_blocks, parent_panel, child_panel)
    parts, products = images_of(masked, inverse, lax.axis_index("zh"))
    parent_column, child_column = columns(parent_blocks, child_blocks, parts, child_top)
    parent_diagonal, child_upper, child_diagonal = finish(*sum_all(products), child_top, diag_parent, diag_child)
    return parent_column, parent_diagonal, child_column, child_upper, child_diagonal


def solution(mesh):
    fine = Mesh(mesh.devices.reshape(4, 2, 2, 4, 2), AXES)
    everywhere = P(AXES, None)
    whole = P(None, None)
    return jax.shard_map(
        local_step,
        mesh=fine,
        in_specs=(P(("y", "zh"), ("zl", "x", "c")), everywhere, everywhere, whole, whole, whole, P(None), P(None)),
        out_specs=(everywhere, whole, everywhere, whole, whole),
        check_vma=False,
    )
```
